128 devices in a mesh: row: 8 (over y, core), col: 16 (over z, x).
Axes of the slice: x: 4, y: 4, z: 4, core: 2. Of those that a mesh axis runs over, the one named last changes fastest.
Arguments:
- covariance: float32 [16384, 16384], P('row', 'col'), as said below
- weights: float32 [16384], P(('row', 'col')), may hold values from 0.5 to 1
- dual_slacks: float32 [16384], P(('row', 'col')), may hold values from 2.5 to 10
- returns: float32 [16384], P(('row', 'col')), may hold values from -6 to 6
- targets: float32 [256], P('col'), may hold values from 0.5 to 1
- sector_duals: float32 [256], replicated, may hold values from -6 to 6
- lengths: int32 [256], replicated, may hold values from 1 to 1024, 16384 in all
Outputs:
- factored: float32 [16384, 16384], P('row', 'col')
- solved_rhs: float32 [16384], P('row')
- sector_cols: float32 [16384, 256], P('row', 'col')
- sector_resid: float32 [256], P('col')
The draws below stay inside these ranges and needn't reach their ends.
Inputs may be any that keep to these rules, and one draw needn't show every extreme that they name: `lengths`: lengths sum to 16384. `covariance`: only the lower triangle with the diagonal is read; with the added diagonal the system is positive definite.
All inputs are finite; a program needn't handle non-finite values.
Results may differ from the reference program's by a relative error of at most 0.0003.
Values sent between devices are 32-bit elements; how exact they have to be, the bound alone decides.
No kernel may reach another device: no remote copies, remote signals or barrier semaphores. Data moves between devices by JAX's collectives and lax.ppermute only.
A program may use at most 128 MiB of HBM per device.

```python
import math
import jax
import jax.numpy as jnp
import numpy as np
from jax import lax

N = 16384
SECT = 256
MOST_LEN = 1024
NB = 128
PANELS = 8


def draw_covariance(key, part):
    factor_count = max(4, min(64, N // 32))
    key_load, key_beta, key_noise = jax.random.split(key, 3)
    loadings = jnp.clip(jax.random.normal(key_load, (N, factor_count), jnp.float32), -4.0, 4.0)
    noise = jnp.clip(jax.random.normal(key_noise, (N, N), jnp.float32), -4.0, 4.0)
    market = 1.0
    betas = jax.random.uniform(key_beta, (N,), jnp.float32, 0.5, 1.5)
    scaled = loadings
    factor_part = jnp.dot(scaled, scaled.T, precision=lax.Precision.HIGHEST) * (0.5 / factor_count)
    market_part = market / N * betas[:, None] * betas[None, :]
    return factor_part + market_part + noise * (1.0 / math.sqrt(N))


def levels(rng, dims, pieces, smallest, high):
    factor_of, own = 1.0, jax.random.fold_in(rng, 6)
    for position, shards_of in pieces:
        steps = jnp.exp(jax.random.uniform(jax.random.fold_in(own, position), (shards_of,), jnp.float32, smallest / len(pieces), high / len(pieces)))
        factor_of = factor_of * jnp.repeat(steps, dims[position] // shards_of).reshape([-1 if axis == position else 1 for axis in range(len(dims))])
    return factor_of


def profile(count, total, reach, slope):
    loads = [(1 << 20) // math.isqrt(standing ** slope) + 1 for standing in range(2, count + 1)]
    spare, counts = total - reach - (count - 1), [1] * (count - 1)
    while spare > 0:
        candidates = [i for i in range(count - 1) if counts[i] < reach]
        mass, left = sum([loads[i] for i in candidates]), spare
        for i in candidates:
            more = min(reach - counts[i], max(1, left * loads[i] // mass), spare)
            counts[i] = counts[i] + more
            spare = spare - more
    return np.array([reach] + counts)


def uneven_parts(key, amount, total, most, skew):
    if amount == 2:
        one = jax.random.randint(key, (), max(1, total - most), min(most, total - 1) + 1)
        return jnp.stack([one, total - one])
    sizes = jnp.asarray(profile(amount, total, most, skew), jnp.int32)
    couples = (amount - 1) // 2
    giver, receiver = sizes[1:1 + 2 * couples:2], sizes[2:2 + 2 * couples:2]
    margin = jnp.minimum(giver - 1, most - receiver)
    moved = jax.random.randint(jax.random.fold_in(key, 1), (couples,), 0, 1 << 20) % (margin + 1)
    sizes = sizes.at[1:1 + 2 * couples:2].set(giver - moved).at[2:2 + 2 * couples:2].set(receiver + moved)
    return sizes[jax.random.permutation(jax.random.fold_in(key, 2), amount)]


def centred(stream_key, shape, spread, reach, cuts=(), held_as=jnp.bfloat16):
    gain = levels(stream_key, shape, cuts, -0.22, 0.18) if cuts else 1.0
    entries = jax.random.normal(stream_key, shape, jnp.float32) * spread * gain
    return jnp.minimum(jnp.maximum(entries, -reach), reach).astype(held_as)


def setup_inputs(seed: int = 0) -> dict:
    key_of = jax.random.split(jax.random.key(seed), 8)
    covariance = draw_covariance(jax.random.fold_in(key_of[7], 71), 0)
    weights = jnp.clip(jnp.exp(math.log(1.0) - 0.6931472 * jax.random.uniform(key_of[1], (N,), jnp.float32) ** levels(key_of[1], (N,), ((0, 128),), -0.2, 0.2)), 0.5, 1.0)
    dual_slacks = jnp.clip(jnp.exp(math.log(10.0) - 1.3862944 * jax.random.uniform(key_of[2], (N,), jnp.float32) ** levels(key_of[2], (N,), ((0, 128),), -0.2, 0.2)), 2.5, 10.0)
    returns = centred(key_of[3], (N,), 1.0, 6.0, ((0, 128),), jnp.float32)
    targets = jnp.clip(0.5 + 0.5 * jax.random.uniform(key_of[4], (SECT,), jnp.float32) ** levels(key_of[4], (SECT,), ((0, 16),), -0.2, 0.2), 0.5, 1.0)
    sector_duals = centred(key_of[5], (SECT,), 1.0, 6.0, (), jnp.float32)
    lengths = uneven_parts(key_of[6], SECT, N, MOST_LEN, 2).astype(jnp.int32)
    return dict(covariance=covariance, weights=weights, dual_slacks=dual_slacks, returns=returns, targets=targets, sector_duals=sector_duals, lengths=lengths)


HIGH = lax.Precision.HIGHEST
SIGMA_GAP = 0.5

def symmetric_product(covariance, weights):
    blocks = 16
    rows_per = covariance.shape[0] // blocks
    stacked = covariance.reshape(blocks, rows_per, covariance.shape[1])
    columns = jnp.arange(covariance.shape[1], dtype=jnp.int32)
    starts = jnp.arange(blocks, dtype=jnp.int32) * rows_per

    def accumulate(column_sum, item):
        tile_block, start_row = item
        row_index = start_row + jnp.arange(rows_per, dtype=jnp.int32)
        lower_part = jnp.where(row_index[:, None] >= columns[None, :], tile_block, 0.0)
        strict = jnp.where(row_index[:, None] > columns[None, :], tile_block, 0.0)
        weight_rows = lax.dynamic_slice_in_dim(weights, start_row, rows_per)
        column_sum = column_sum + jnp.dot(weight_rows, strict, precision=HIGH)
        return (column_sum, jnp.dot(lower_part, weights, precision=HIGH))
    column_sum, row_parts = lax.scan(accumulate, jnp.zeros((covariance.shape[1],), jnp.float32), (stacked, starts))
    return column_sum + row_parts.reshape(-1)

def reference(covariance, weights, dual_slacks, returns, targets, sector_duals, lengths):
    sector_ends = jnp.cumsum(lengths).astype(jnp.int32)
    offsets = sector_ends - lengths
    assets = jnp.arange(N, dtype=jnp.int32)
    member = ((assets[:, None] >= offsets[None, :]) & (assets[:, None] < sector_ends[None, :])).astype(jnp.float32)
    sector_sizes = lengths.astype(jnp.float32)
    sector_resid = targets - jnp.dot(weights, member, precision=HIGH) / sector_sizes
    mean_gap = jnp.sum(weights * dual_slacks) / N
    product = symmetric_product(covariance, weights)
    prices = jnp.dot(member, sector_duals, precision=HIGH)
    rhs = returns - product - prices + SIGMA_GAP * mean_gap / weights
    extras = jnp.concatenate([rhs[:, None], member / jnp.sqrt(sector_sizes)[None, :]], axis=1)
    split = PANELS * NB
    diag_term = dual_slacks / weights
    head = covariance[:split, :split]
    head_index = jnp.arange(split, dtype=jnp.int32)
    head_lower = jnp.tril(head).at[head_index, head_index].add(diag_term[:split])
    head_sym = head_lower + jnp.tril(head, -1).T
    factor_head = jnp.linalg.cholesky(head_sym)
    inverse_head = lax.linalg.triangular_solve(factor_head, jnp.eye(split, dtype=jnp.float32), left_side=True, lower=True)
    factor_tail = jnp.dot(covariance[split:, :split], inverse_head.T, precision=HIGH)
    tail_index = jnp.arange(N - split, dtype=jnp.int32)
    schur = covariance[split:, split:] - jnp.dot(factor_tail, factor_tail.T, precision=HIGH)
    schur = schur.at[tail_index, tail_index].add(diag_term[split:])
    solved_head = jnp.dot(inverse_head, extras[:split], precision=HIGH)
    solved_tail = extras[split:] - jnp.dot(factor_tail, solved_head, precision=HIGH)
    top = jnp.concatenate([jnp.tril(factor_head), jnp.zeros((split, N - split), jnp.float32)], axis=1)
    bottom = jnp.concatenate([factor_tail, jnp.tril(schur)], axis=1)
    factored = jnp.concatenate([top, bottom], axis=0)
    solved = jnp.concatenate([solved_head, solved_tail], axis=0)
    return (factored, solved[:, 0], solved[:, 1:], sector_resid)
```

```python
import functools

import jax
import jax.numpy as jnp
from jax import lax
from jax.experimental import pallas as pl
from jax.experimental.pallas import tpu as pltpu
from jax.sharding import Mesh
from jax.sharding import PartitionSpec as P

NB = 128
PANELS = 8
LEAD = NB * PANELS
ROW = ("y", "core")
COL = ("z", "x")
ALL = ROW + COL
SIGMA_GAP = 0.5

NN = (((1,), (0,)), ((), ()))
NT = (((1,), (1,)), ((), ()))


def split2(x):
    hi = x.astype(jnp.bfloat16)
    lo = (x - hi.astype(jnp.float32)).astype(jnp.bfloat16)
    return hi, lo


def dot3(a, b, dims):
    ah, al = a
    bh, bl = b
    f = functools.partial(
        lax.dot_general, dimension_numbers=dims, preferred_element_type=jnp.float32
    )
    return f(ah, bh) + (f(ah, bl) + f(al, bh))


def factor_block(d_ref, r_ref):
    lane = lax.broadcasted_iota(jnp.int32, (8, NB), 1)
    sub = lax.broadcasted_iota(jnp.int32, (8, NB), 0)
    wide = lambda x: jnp.broadcast_to(x, (8, NB))
    for g in range(NB // 8):
        base = 8 * g
        head = d_ref[base : base + 8, :]
        cols = [wide(head[:, base + k : base + k + 1]) for k in range(8)]
        out = jnp.zeros((8, NB), jnp.float32)
        scale = jnp.zeros((8, NB), jnp.float32)
        for k in range(8):
            r = lax.rsqrt(wide(cols[k][k : k + 1, :]))
            rp = r * r
            m = jnp.where(sub == k, 0.0, cols[k] * rp)
            here = lane == base + k
            row = jnp.where(here, 1.0, wide(head[k : k + 1, :]))
            out = jnp.where(sub == k, row * r, out)
            scale = jnp.where(sub == k, rp, scale)
            head = jnp.where(here, jnp.where(sub == k, 1.0, 0.0), head) - m * row
            for k2 in range(k + 1, 8):
                cols[k2] = cols[k2] - m * wide(cols[k2][k : k + 1, :])
        r_ref[base : base + 8, :] = out
        head = head * scale
        rows = [wide(head[k : k + 1, :]) for k in range(8)]
        block = (lane >= base) & (lane < base + 8)
        for i in range(g + 1, NB // 8):
            cur = d_ref[8 * i : 8 * i + 8, :]
            t = [wide(cur[:, base + k : base + k + 1]) * rows[k] for k in range(8)]
            t = ((t[0] + t[1]) + (t[2] + t[3])) + ((t[4] + t[5]) + (t[6] + t[7]))
            d_ref[8 * i : 8 * i + 8, :] = jnp.where(block, 0.0, cur) - t


def stacked(pair, axis):
    return jnp.concatenate(pair, axis=axis)


def panel_steps(first, last, panels, diag_ref, l_ref, w_ref, d_ref, r_ref):
    n = panels * NB
    ri = lax.broadcasted_iota(jnp.int32, (NB, NB), 0)
    ci = lax.broadcasted_iota(jnp.int32, (NB, NB), 1)
    f = lambda a, b, dims: lax.dot_general(a, b, dims, preferred_element_type=jnp.float32)

    def step(kb, _):
        at = pl.multiple_of(kb * NB, NB)
        d = w_ref[pl.ds(at, NB), pl.ds(at, NB)]
        added = jnp.where(ri == ci, jnp.broadcast_to(diag_ref[pl.ds(kb, 1), :], (NB, NB)), 0.0)
        d_ref[...] = jnp.where(ri >= ci, d, d.T) + added
        factor_block(d_ref, r_ref)
        both = r_ref[...]
        inv = jnp.where(ri >= ci, both, 0.0)
        up = jnp.where(ri < ci, both, jnp.where(ri == ci, 1.0 / both, 0.0))
        l_ref[pl.ds(at, NB), pl.ds(at, NB)] = up.T
        invs = split2(inv)
        for k in range(first, last):

            @pl.when(kb == k)
            def _():
                lo, hi = k * NB, (k + 1) * NB
                if k:
                    w_ref[lo:hi, :lo] = dot3(invs, split2(w_ref[lo:hi, :lo]), NN)
                w_ref[lo:hi, lo:hi] = inv
                if k < panels - 1:
                    low = dot3(split2(w_ref[hi:, lo:hi]), invs, NT)
                    l_ref[hi:, lo:hi] = low
                    l_ref[lo:hi, hi:] = jnp.zeros((NB, n - hi), jnp.float32)
                    w_ref[lo:hi, hi:] = jnp.zeros((NB, n - hi), jnp.float32)
                    lh, ll = split2(low)
                    both_l, twice_l = stacked((lh, ll), 1), stacked((lh, lh), 1)
                    wh, wl = split2(w_ref[lo:hi, :hi])
                    t = f(both_l, stacked((wh, wh), 0), NN) + f(lh, wl, NN)
                    if k:
                        w_ref[hi:, :lo] -= t[:, :lo]
                    w_ref[hi:, lo:hi] = -t[:, lo:]
                    for c in range(hi, n, 2 * NB):
                        a0, a1 = c - hi, min(c + 2 * NB, n) - hi
                        t = f(both_l[a0:], twice_l[a0:a1], NT) + f(lh[a0:], ll[a0:a1], NT)
                        w_ref[c:, c : hi + a1] -= t

        return 0

    lax.fori_loop(first, last, step, 0)


def chol_start(panels, last, mine_ref, other_ref, diag_ref, l_ref, w_ref, d_ref, r_ref):
    core = lax.axis_index("core")
    span = mine_ref.shape[0]

    @pl.when(core == 0)
    def _():
        w_ref[:span] = mine_ref[...]
        w_ref[span:] = other_ref[...]

    @pl.when(core == 1)
    def _():
        w_ref[:span] = other_ref[...]
        w_ref[span:] = mine_ref[...]

    panel_steps(0, last, panels, diag_ref, l_ref, w_ref, d_ref, r_ref)


def chol_rest(panels, first, l_in, w_in, diag_ref, l_ref, w_ref, d_ref, r_ref):
    l_ref[...] = l_in[...]
    w_ref[...] = w_in[...]
    panel_steps(first, panels, panels, diag_ref, l_ref, w_ref, d_ref, r_ref)


def chol_part(kernel, *args):
    n = args[0].shape[1]
    return pl.pallas_call(
        kernel,
        out_shape=[jax.ShapeDtypeStruct((n, n), jnp.float32)] * 2,
        in_specs=[pl.BlockSpec(memory_space=pltpu.VMEM)] * 3,
        out_specs=[pl.BlockSpec(memory_space=pltpu.VMEM)] * 2,
        scratch_shapes=[pltpu.VMEM((NB, NB), jnp.float32)] * 2,
        compiler_params=pltpu.CompilerParams(vmem_limit_bytes=50 * 2**20),
    )(*args)


SPLIT_AT = 3


def flat(y, core, z, x):
    return ((y * 2 + core) * 4 + z) * 4 + x


def factor_kernel(w_ref, own_ref, other_ref, e_ref, xh_ref, xl_ref, g_ref, head_ref, ah, al, mh, ml):
    n, wide = LEAD, 256
    core, y, col = lax.axis_index("core"), lax.axis_index("y"), lax.axis_index(COL)
    piece = own_ref.shape[1]
    for k in range(4):
        group = 2 * lax.rem(y - k + 4, 4)
        for source, q in ((own_ref, core), (other_ref, 1 - core)):
            hi, lo = split2(source[k])
            at = pl.multiple_of((group + q) * piece, piece)
            ah[pl.ds(at, piece), :] = hi
            al[pl.ds(at, piece), :] = lo
    eh, el = split2(e_ref[...])
    ri = lax.broadcasted_iota(jnp.int32, (wide, n), 0)
    ci = lax.broadcasted_iota(jnp.int32, (wide, n), 1)
    for i in range(n // wide):
        lo, hi = i * wide, (i + 1) * wide
        w = split2(w_ref[lo:hi, :hi])
        m = dot3(w, (ah[:, :hi], al[:, :hi]), NT)
        m = jnp.where(col == 0, jnp.where(ri + lo == ci, -1.0, 0.0), m)
        mh[lo:hi, :n], ml[lo:hi, :n] = split2(m)
        m = dot3(w, (eh[:hi], el[:hi]), NN)
        head_ref[lo:hi, :] = m
        mh[lo:hi, n:], ml[lo:hi, n:] = split2(m)
    for i in range(n // wide):
        lo, hi = i * wide, (i + 1) * wide
        w = split2(w_ref[lo:, lo:hi].T)
        x = dot3(w, (mh[lo:, :], ml[lo:, :]), NN)
        xh_ref[lo:hi, :], xl_ref[lo:hi, :] = split2(x[:, :n])
        gh, gl = split2(x[:, n:])
        g_ref[lo:hi, :64], g_ref[lo:hi, 64:] = gh[:, :64], gl[:, :64]


def weigh(inverse, own, other, extra):
    n = inverse.shape[0]
    vmem = pl.BlockSpec(memory_space=pltpu.VMEM)
    return pl.pallas_call(
        factor_kernel,
        out_shape=[
            jax.ShapeDtypeStruct((n, n), jnp.bfloat16),
            jax.ShapeDtypeStruct((n, n), jnp.bfloat16),
            jax.ShapeDtypeStruct((n, NB), jnp.bfloat16),
            jax.ShapeDtypeStruct((n, NB), jnp.float32),
        ],
        in_specs=[vmem] * 4,
        out_specs=[vmem] * 4,
        scratch_shapes=[pltpu.VMEM((n, n), jnp.bfloat16)] * 2
        + [pltpu.VMEM((n, n + NB), jnp.bfloat16)] * 2,
        compiler_params=pltpu.CompilerParams(vmem_limit_bytes=56 * 2**20),
        name="weigh",
    )(inverse, own, other, extra)


def update_kernel(rows_ref, xh_ref, xl_ref, g_ref, cov_ref, low_ref, e_ref, head_ref, d_ref, out_ref, rhs_ref, sec_ref):
    block, n = rows_ref.shape
    step = pl.program_id(0)
    rows_total = pl.num_programs(0) * block
    row, col = lax.axis_index(ROW), lax.axis_index(COL)
    ah, al = split2(rows_ref[...])
    x = (xh_ref[...], xl_ref[...])
    t = dot3((ah, al), x, NN)
    f = functools.partial(
        lax.dot_general, dimension_numbers=NN, preferred_element_type=jnp.float32
    )
    g = g_ref[...]
    p, q = f(ah, g), f(al, g)
    extra = e_ref[...] - (p[:, :64] + (p[:, 64:] + q[:, :64]))
    top = (row == 0) & (step * block < LEAD)
    extra = jnp.where(top, head_ref[:, :64], extra)
    sec_ref[...] = extra[:, 1 : 1 + sec_ref.shape[1]]
    rhs_ref[...] = jnp.concatenate([extra, jnp.zeros_like(extra)], axis=1).T[0:1, :]
    ri = lax.broadcasted_iota(jnp.int32, (block, n), 0) + (row * rows_total + step * block)
    ci = lax.broadcasted_iota(jnp.int32, (block, n), 1) + col * n
    base = jnp.where(ri == ci, cov_ref[...] + d_ref[...], cov_ref[...])
    base = jnp.where(col == 0, 0.0, base)
    tile = jnp.where(ri >= ci, base - t, 0.0)
    out_ref[...] = jnp.where(top & (col == 0), low_ref[...], tile)


def update(rows, xh, xl, g, covariance, lower, extra, head, diag, sectors):
    m, n = covariance.shape
    block = 256
    last = LEAD // block - 1
    whole = lambda a: pl.BlockSpec(a.shape, lambda i: (0, 0))
    lines = lambda w: pl.BlockSpec((block, w), lambda i: (i, 0))
    ahead = lambda w: pl.BlockSpec((block, w), lambda i: (jnp.minimum(i, last), 0))
    return pl.pallas_call(
        update_kernel,
        grid=(m // block,),
        out_shape=[
            jax.ShapeDtypeStruct((m, n), jnp.float32),
            jax.ShapeDtypeStruct((1, m), jnp.float32),
            jax.ShapeDtypeStruct((m, sectors), jnp.float32),
        ],
        in_specs=[lines(n), whole(xh), whole(xl), whole(g), lines(n), ahead(n), lines(64), ahead(NB), whole(diag)],
        out_specs=[lines(n), pl.BlockSpec((1, block), lambda i: (0, i)), lines(sectors)],
        compiler_params=pltpu.CompilerParams(
            vmem_limit_bytes=56 * 2**20, dimension_semantics=("arbitrary",)
        ),
        name="update",
    )(rows, xh, xl, g, covariance, lower, extra, head, diag)


def place(y, core, near, far):
    return flat(y, core, far, near) if core == 0 else flat(y, core, near, far)


def spread_lead(half, wait_far, wait_all, wait_near):
    first = lax.axis_index("core") == 0
    z, x, y = lax.axis_index("z"), lax.axis_index("x"), lax.axis_index("y")
    near, far = jnp.where(first, x, z), jnp.where(first, z, x)
    four = range(4)
    cores = range(2)
    loads = half.reshape(4, -1, LEAD)
    bundle = loads[0]
    for k in range(1, 4):
        got = lax.ppermute(loads[k], ALL, [(place(0, c, 0, 0), place(0, c, k, 0)) for c in cores])
        bundle = jnp.where(near == k, got, bundle)
    bundle, far_done = wait_far(bundle)
    loads = bundle.reshape(4, -1, LEAD)
    part = loads[0]
    for k in range(1, 4):
        pairs = [(place(0, c, n, 0), place(0, c, n, k)) for c in cores for n in four]
        part = jnp.where(far == k, lax.ppermute(loads[k], ALL, pairs), part)
    own = part
    for k in range(1, 4):
        pairs = [(place(0, c, n, f), place(k, c, n, f)) for c in cores for n in four for f in four]
        own = jnp.where(y == k, lax.ppermute(part, ALL, pairs), own)
    own, all_done = wait_all(own, far_done)

    def exchange(block, index, ahead):
        out = lax.dynamic_update_slice_in_dim(
            jnp.zeros((4,) + block.shape, block.dtype), block[None], index, 0
        )
        for k in range(1, 4):
            got = lax.ppermute(block, ALL, ahead(k))
            out = lax.dynamic_update_slice_in_dim(out, got[None], lax.rem(index - k + 4, 4), 0)
        return out.reshape(-1, LEAD)

    def along_far(k):
        return [
            (place(v, c, n, f), place(v, c, n, (f + k) % 4)) for v in four for c in cores for n in four for f in four
        ]

    def along_near(k):
        return [
            (place(v, c, n, f), place(v, c, (n + k) % 4, f)) for v in four for c in cores for n in four for f in four
        ]

    own = exchange(own, far, along_far)
    near_done = wait_near(own, all_done)
    return exchange(own, near, along_near), near_done


def on_device(covariance, weights, dual_slacks, returns, targets, sector_duals, lengths):
    tile_rows, tile_cols = covariance.shape
    rows_n, cols_n = 8, 16
    order = tile_rows * rows_n
    row_id, col_id = lax.axis_index(ROW), lax.axis_index(COL)
    row_start, col_start = row_id * tile_rows, col_id * tile_cols
    sectors_here = targets.shape[0]
    global_rows = row_start + jnp.arange(tile_rows, dtype=jnp.int32)
    global_cols = col_start + jnp.arange(tile_cols, dtype=jnp.int32)

    panel, small = lax.optimization_barrier(
        (jnp.where(col_id == 0, covariance, 0.0), jnp.stack([weights, dual_slacks, returns]))
    )
    own = lax.psum_scatter(panel, COL, scatter_dimension=0, tiled=True)
    small = lax.all_gather(small, COL, axis=0, tiled=True)
    lower_mask = global_rows[:, None] >= global_cols[None, :]
    strict_mask = global_rows[:, None] > global_cols[None, :]

    def gather_all(value, small):
        value, small = lax.optimization_barrier((value, small))
        small = lax.all_gather(small, ROW, axis=0, tiled=True).reshape(rows_n * cols_n, 3, -1)
        return lax.optimization_barrier((value, [small[:, k].reshape(order) for k in range(3)]))

    def partial_sums(value, vectors):
        value, vectors = lax.optimization_barrier((value, vectors))
        del value
        weight_rows = lax.dynamic_slice_in_dim(vectors[0], row_start, tile_rows)
        weight_cols = lax.dynamic_slice_in_dim(vectors[0], col_start, tile_cols)
        row_part = jnp.sum(jnp.where(lower_mask, covariance, 0.0) * weight_cols[None, :], axis=1)
        col_part = jnp.sum(jnp.where(strict_mask, covariance, 0.0) * weight_rows[:, None], axis=0)
        lines = jnp.concatenate([col_part, row_part[:LEAD]]).reshape(1, -1)
        return vectors, row_part, lax.all_gather(lines, ROW, axis=0, tiled=True)

    half = LEAD // 2
    second = lax.ppermute(covariance[half:LEAD], ALL, [(flat(0, 0, 0, 0), flat(0, 1, 0, 0))])
    mine, held = spread_lead(
        jnp.where(lax.axis_index("core") == 0, covariance[:half], second),
        lambda value: lax.optimization_barrier((value, small)),
        gather_all,
        partial_sums,
    )
    (full_weights, full_slacks, full_returns), row_part, lines = held
    own, mine = lax.optimization_barrier((own, mine))
    moved = lax.ppermute(
        own, ALL, [(g, (g % rows_n) * cols_n + g // rows_n) for g in range(rows_n * cols_n)]
    )
    col_sum, head_part = jnp.sum(lines[:, :tile_cols], axis=0), lines[0, tile_cols:]
    left = row_part[:tile_cols] + jnp.where(col_id == 2 * row_id, col_sum, 0.0)
    right = row_part[tile_cols:] + jnp.where(col_id == 2 * row_id + 1, col_sum, 0.0)
    head_part = head_part + jnp.where(col_id == 0, col_sum, 0.0)
    lines = jnp.stack([left, right, head_part] + [jnp.zeros_like(left)] * 13)
    lines = lax.all_gather(lines, COL, axis=0, tiled=True)
    row_lines = lax.all_gather(own, COL, axis=0, tiled=True)
    around = [moved]
    for k in range(1, 4):
        around.append(lax.ppermute(moved, "y", [(v, (v + k) % 4) for v in range(4)]))
    diag = full_slacks / full_weights
    mean_gap = jnp.sum(full_weights * full_slacks) / order

    head_index = jnp.arange(LEAD, dtype=jnp.int32)
    other = lax.ppermute(mine, "core", [(0, 1), (1, 0)])
    head_diag = diag[:LEAD].reshape(PANELS, NB)
    lower, inverse = chol_part(
        functools.partial(chol_start, PANELS, SPLIT_AT), mine, other, head_diag
    )
    lower, inverse = chol_part(
        functools.partial(chol_rest, PANELS, SPLIT_AT), lower, inverse, head_diag
    )
    around, inverse = lax.optimization_barrier((jnp.stack(around), inverse))
    across = lax.ppermute(around, "core", [(0, 1), (1, 0)])
    product = jnp.sum(lines.reshape(cols_n, 16, -1)[:, :3], axis=0).reshape(-1)

    sector_ends = jnp.cumsum(lengths)
    offsets = sector_ends - lengths
    sector_index = col_id * sectors_here + jnp.arange(sectors_here, dtype=jnp.int32)
    my_offsets, my_ends = jnp.take(offsets, sector_index), jnp.take(sector_ends, sector_index)
    my_sizes = jnp.take(lengths, sector_index).astype(jnp.float32)
    assets = jnp.arange(order, dtype=jnp.int32)
    inside = (assets[None, :] >= my_offsets[:, None]) & (assets[None, :] < my_ends[:, None])
    sector_resid = targets - jnp.sum(jnp.where(inside, full_weights[None, :], 0.0), axis=1) / my_sizes

    def extras(index, start, count, product_here):
        member = (index[:, None] >= offsets[None, :]) & (index[:, None] < sector_ends[None, :])
        prices = jnp.sum(jnp.where(member, sector_duals[None, :], 0.0), axis=1)
        w = lax.dynamic_slice_in_dim(full_weights, start, count)
        ret = lax.dynamic_slice_in_dim(full_returns, start, count)
        rhs = ret - product_here - prices + SIGMA_GAP * mean_gap / w
        mine = (index[:, None] >= my_offsets[None, :]) & (index[:, None] < my_ends[None, :])
        sectors = jnp.where(mine, lax.rsqrt(my_sizes)[None, :], 0.0)
        return jnp.concatenate(
            [rhs[:, None], sectors, jnp.zeros((count, 47), jnp.float32)], axis=1
        )

    head = extras(head_index, 0, LEAD, product[tile_rows:])
    body = extras(global_rows, row_start, tile_rows, product[:tile_rows])
    head = jnp.concatenate([head, jnp.zeros_like(head)], axis=1)
    xh, xl, g, solved_head = weigh(inverse, around, across, head)
    diag_cols = lax.dynamic_slice_in_dim(diag, col_start, tile_cols)[None, :]
    factored, rhs, sector_cols = update(
        row_lines, xh, xl, g, covariance, lower, body, solved_head, diag_cols, sectors_here
    )
    return factored, rhs.reshape(tile_rows), sector_cols, sector_resid


def solution(mesh):
    finer = Mesh(mesh.devices.reshape(4, 2, 4, 4), ALL)
    in_specs = (P(ROW, COL), P(ALL), P(ALL), P(ALL), P(COL), P(), P())
    out_specs = (P(ROW, COL), P(ROW), P(ROW, COL), P(COL))
    return jax.shard_map(
        on_device, mesh=finer, in_specs=in_specs, out_specs=out_specs, check_vma=False
    )
```

```python
import functools

import jax
import jax.numpy as jnp
from jax import lax
from jax.experimental import pallas as pl
from jax.experimental.pallas import tpu as pltpu
from jax.sharding import Mesh
from jax.sharding import PartitionSpec as P

NB = 128
PANELS = 8
LEAD = NB * PANELS
ROW = ("y", "core")
COL = ("z", "x")
ALL = ROW + COL
SIGMA_GAP = 0.5

NN = (((1,), (0,)), ((), ()))
NT = (((1,), (1,)), ((), ()))


def split2(x):
    hi = x.astype(jnp.bfloat16)
    lo = (x - hi.astype(jnp.float32)).astype(jnp.bfloat16)
    return hi, lo


def dot3(a, b, dims):
    ah, al = a
    bh, bl = b
    f = functools.partial(
        lax.dot_general, dimension_numbers=dims, preferred_element_type=jnp.float32
    )
    return f(ah, bh) + (f(ah, bl) + f(al, bh))


def factor_block(d_ref, r_ref):
    lane = lax.broadcasted_iota(jnp.int32, (8, NB), 1)
    sub = lax.broadcasted_iota(jnp.int32, (8, NB), 0)
    wide = lambda x: jnp.broadcast_to(x, (8, NB))
    for g in range(NB // 8):
        base = 8 * g
        head = d_ref[base : base + 8, :]
        cols = [
            jnp.where(lane == base + k, head, wide(head[:, base + k : base + k + 1])) for k in range(8)
        ]
        out = jnp.zeros((8, NB), jnp.float32)
        scale = jnp.zeros((8, NB), jnp.float32)
        for k in range(8):
            r = lax.rsqrt(wide(cols[k][k : k + 1, :]))
            rp = r * r
            m = jnp.where(sub == k, 0.0, cols[k] * rp)
            here = lane == base + k
            row = jnp.where(here, 1.0, wide(head[k : k + 1, :]))
            out = jnp.where(sub == k, row * r, out)
            scale = jnp.where(sub == k, rp, scale)
            head = jnp.where(here, jnp.where(sub == k, 1.0, 0.0), head) - m * row
            for k2 in range(k + 1, 8):
                cols[k2] = cols[k2] - m * wide(cols[k2][k : k + 1, :])
        r_ref[base : base + 8, :] = out
        head = head * scale
        rows = [wide(head[k : k + 1, :]) for k in range(8)]
        block = (lane >= base) & (lane < base + 8)
        for i in range(g + 1, NB // 8):
            cur = d_ref[8 * i : 8 * i + 8, :]
            t = [wide(cur[:, base + k : base + k + 1]) * rows[k] for k in range(8)]
            t = ((t[0] + t[1]) + (t[2] + t[3])) + ((t[4] + t[5]) + (t[6] + t[7]))
            d_ref[8 * i : 8 * i + 8, :] = jnp.where(block, 0.0, cur) - t


def stacked(pair, axis):
    return jnp.concatenate(pair, axis=axis)


def panel_steps(first, last, panels, diag_ref, l_ref, w_ref, d_ref, r_ref):
    n = panels * NB
    ri = lax.broadcasted_iota(jnp.int32, (NB, NB), 0)
    ci = lax.broadcasted_iota(jnp.int32, (NB, NB), 1)
    f = lambda a, b, dims: lax.dot_general(a, b, dims, preferred_element_type=jnp.float32)

    def step(kb, _):
        at = pl.multiple_of(kb * NB, NB)
        d = w_ref[pl.ds(at, NB), pl.ds(at, NB)]
        added = jnp.where(ri == ci, jnp.broadcast_to(diag_ref[pl.ds(kb, 1), :], (NB, NB)), 0.0)
        d_ref[...] = jnp.where(ri >= ci, d, d.T) + added
        factor_block(d_ref, r_ref)
        both = r_ref[...]
        inv = jnp.where(ri >= ci, both, 0.0)
        up = jnp.where(ri < ci, both, jnp.where(ri == ci, 1.0 / both, 0.0))
        l_ref[pl.ds(at, NB), pl.ds(at, NB)] = up.T
        invs = split2(inv)
        for k in range(first, last):

            @pl.when(kb == k)
            def _():
                lo, hi = k * NB, (k + 1) * NB
                if k:
                    w_ref[lo:hi, :lo] = dot3(invs, split2(w_ref[lo:hi, :lo]), NN)
                w_ref[lo:hi, lo:hi] = inv
                if k < panels - 1:
                    low = dot3(split2(w_ref[hi:, lo:hi]), invs, NT)
                    l_ref[hi:, lo:hi] = low
                    l_ref[lo:hi, hi:] = jnp.zeros((NB, n - hi), jnp.float32)
                    w_ref[lo:hi, hi:] = jnp.zeros((NB, n - hi), jnp.float32)
                    lh, ll = split2(low)
                    both_l, twice_l = stacked((lh, ll), 1), stacked((lh, lh), 1)
                    wh, wl = split2(w_ref[lo:hi, :hi])
                    t = f(both_l, stacked((wh, wh), 0), NN) + f(lh, wl, NN)
                    if k:
                        w_ref[hi:, :lo] -= t[:, :lo]
                    w_ref[hi:, lo:hi] = -t[:, lo:]
                    for c in range(hi, n, 2 * NB):
                        a0, a1 = c - hi, min(c + 2 * NB, n) - hi
                        t = f(both_l[a0:], twice_l[a0:a1], NT) + f(lh[a0:], ll[a0:a1], NT)
                        w_ref[c:, c : hi + a1] -= t

        return 0

    lax.fori_loop(first, last, step, 0)


def chol_start(panels, last, mine_ref, other_ref, diag_ref, l_ref, w_ref, d_ref, r_ref):
    core = lax.axis_index("core")
    span = mine_ref.shape[0]

    @pl.when(core == 0)
    def _():
        w_ref[:span] = mine_ref[...]
        w_ref[span:] = other_ref[...]

    @pl.when(core == 1)
    def _():
        w_ref[:span] = other_ref[...]
        w_ref[span:] = mine_ref[...]

    panel_steps(0, last, panels, diag_ref, l_ref, w_ref, d_ref, r_ref)


def chol_rest(panels, first, l_in, w_in, diag_ref, l_ref, w_ref, d_ref, r_ref):
    l_ref[...] = l_in[...]
    w_ref[...] = w_in[...]
    panel_steps(first, panels, panels, diag_ref, l_ref, w_ref, d_ref, r_ref)


def chol_part(kernel, *args):
    n = args[0].shape[1]
    return pl.pallas_call(
        kernel,
        out_shape=[jax.ShapeDtypeStruct((n, n), jnp.float32)] * 2,
        in_specs=[pl.BlockSpec(memory_space=pltpu.VMEM)] * 3,
        out_specs=[pl.BlockSpec(memory_space=pltpu.VMEM)] * 2,
        scratch_shapes=[pltpu.VMEM((NB, NB), jnp.float32)] * 2,
        compiler_params=pltpu.CompilerParams(vmem_limit_bytes=50 * 2**20),
    )(*args)


SPLIT_AT = 3


def flat(y, core, z, x):
    return ((y * 2 + core) * 4 + z) * 4 + x


def factor_kernel(w_ref, own_ref, other_ref, e_ref, xh_ref, xl_ref, g_ref, head_ref, ah, al, mh, ml):
    n, wide = LEAD, 256
    core, y, col = lax.axis_index("core"), lax.axis_index("y"), lax.axis_index(COL)
    piece = own_ref.shape[1]
    for k in range(4):
        group = 2 * lax.rem(y - k + 4, 4)
        for source, q in ((own_ref, core), (other_ref, 1 - core)):
            hi, lo = split2(source[k])
            at = pl.multiple_of((group + q) * piece, piece)
            ah[pl.ds(at, piece), :] = hi
            al[pl.ds(at, piece), :] = lo
    eh, el = split2(e_ref[...])
    ri = lax.broadcasted_iota(jnp.int32, (wide, n), 0)
    ci = lax.broadcasted_iota(jnp.int32, (wide, n), 1)
    for i in range(n // wide):
        lo, hi = i * wide, (i + 1) * wide
        w = split2(w_ref[lo:hi, :hi])
        m = dot3(w, (ah[:, :hi], al[:, :hi]), NT)
        m = jnp.where(col == 0, jnp.where(ri + lo == ci, -1.0, 0.0), m)
        mh[lo:hi, :n], ml[lo:hi, :n] = split2(m)
        m = dot3(w, (eh[:hi], el[:hi]), NN)
        head_ref[lo:hi, :] = m
        mh[lo:hi, n:], ml[lo:hi, n:] = split2(m)
    for i in range(n // wide):
        lo, hi = i * wide, (i + 1) * wide
        w = split2(w_ref[lo:, lo:hi].T)
        x = dot3(w, (mh[lo:, :], ml[lo:, :]), NN)
        xh_ref[lo:hi, :], xl_ref[lo:hi, :] = split2(x[:, :n])
        gh, gl = split2(x[:, n:])
        g_ref[lo:hi, :64], g_ref[lo:hi, 64:] = gh[:, :64], gl[:, :64]


def weigh(inverse, own, other, extra):
    n = inverse.shape[0]
    vmem = pl.BlockSpec(memory_space=pltpu.VMEM)
    return pl.pallas_call(
        factor_kernel,
        out_shape=[
            jax.ShapeDtypeStruct((n, n), jnp.bfloat16),
            jax.ShapeDtypeStruct((n, n), jnp.bfloat16),
            jax.ShapeDtypeStruct((n, NB), jnp.bfloat16),
            jax.ShapeDtypeStruct((n, NB), jnp.float32),
        ],
        in_specs=[vmem] * 4,
        out_specs=[vmem] * 4,
        scratch_shapes=[pltpu.VMEM((n, n), jnp.bfloat16)] * 2
        + [pltpu.VMEM((n, n + NB), jnp.bfloat16)] * 2,
        compiler_params=pltpu.CompilerParams(vmem_limit_bytes=56 * 2**20),
        name="weigh",
    )(inverse, own, other, extra)


def update_kernel(rows_ref, xh_ref, xl_ref, g_ref, cov_ref, low_ref, e_ref, head_ref, d_ref, out_ref, rhs_ref, sec_ref):
    block, n = rows_ref.shape
    step = pl.program_id(0)
    rows_total = pl.num_programs(0) * block
    row, col = lax.axis_index(ROW), lax.axis_index(COL)
    ah, al = split2(rows_ref[...])
    x = (xh_ref[...], xl_ref[...])
    t = dot3((ah, al), x, NN)
    f = functools.partial(
        lax.dot_general, dimension_numbers=NN, preferred_element_type=jnp.float32
    )
    g = g_ref[...]
    p, q = f(ah, g), f(al, g)
    extra = e_ref[...] - (p[:, :64] + (p[:, 64:] + q[:, :64]))
    top = (row == 0) & (step * block < LEAD)
    extra = jnp.where(top, head_ref[:, :64], extra)
    sec_ref[...] = extra[:, 1 : 1 + sec_ref.shape[1]]
    rhs_ref[...] = jnp.concatenate([extra, jnp.zeros_like(extra)], axis=1).T[0:1, :]
    ri = lax.broadcasted_iota(jnp.int32, (block, n), 0) + (row * rows_total + step * block)
    ci = lax.broadcasted_iota(jnp.int32, (block, n), 1) + col * n
    base = jnp.where(ri == ci, cov_ref[...] + d_ref[...], cov_ref[...])
    base = jnp.where(col == 0, 0.0, base)
    tile = jnp.where(ri >= ci, base - t, 0.0)
    out_ref[...] = jnp.where(top & (col == 0), low_ref[...], tile)


def update(rows, xh, xl, g, covariance, lower, extra, head, diag, sectors):
    m, n = covariance.shape
    block = 256
    last = LEAD // block - 1
    whole = lambda a: pl.BlockSpec(a.shape, lambda i: (0, 0))
    lines = lambda w: pl.BlockSpec((block, w), lambda i: (i, 0))
    ahead = lambda w: pl.BlockSpec((block, w), lambda i: (jnp.minimum(i, last), 0))
    return pl.pallas_call(
        update_kernel,
        grid=(m // block,),
        out_shape=[
            jax.ShapeDtypeStruct((m, n), jnp.float32),
            jax.ShapeDtypeStruct((1, m), jnp.float32),
            jax.ShapeDtypeStruct((m, sectors), jnp.float32),
        ],
        in_specs=[lines(n), whole(xh), whole(xl), whole(g), lines(n), ahead(n), lines(64), ahead(NB), whole(diag)],
        out_specs=[lines(n), pl.BlockSpec((1, block), lambda i: (0, i)), lines(sectors)],
        compiler_params=pltpu.CompilerParams(
            vmem_limit_bytes=56 * 2**20, dimension_semantics=("arbitrary",)
        ),
        name="update",
    )(rows, xh, xl, g, covariance, lower, extra, head, diag)


def place(y, core, near, far):
    return flat(y, core, far, near) if core == 0 else flat(y, core, near, far)


def spread_lead(half, panel):
    first = lax.axis_index("core") == 0
    z, x, y = lax.axis_index("z"), lax.axis_index("x"), lax.axis_index("y")
    near, far = jnp.where(first, x, z), jnp.where(first, z, x)
    four = range(4)
    cores = range(2)
    loads = half.reshape(4, -1, LEAD)
    bundle = loads[0]
    for k in range(1, 4):
        got = lax.ppermute(loads[k], ALL, [(place(0, c, 0, 0), place(0, c, k, 0)) for c in cores])
        bundle = jnp.where(near == k, got, bundle)
    loads = bundle.reshape(4, -1, LEAD)
    part = loads[0]
    for k in range(1, 4):
        pairs = [(place(0, c, n, 0), place(0, c, n, k)) for c in cores for n in four]
        part = jnp.where(far == k, lax.ppermute(loads[k], ALL, pairs), part)
    own = part
    for k in range(1, 4):
        pairs = [(place(0, c, n, f), place(k, c, n, f)) for c in cores for n in four for f in four]
        own = jnp.where(y == k, lax.ppermute(part, ALL, pairs), own)

    def exchange(block, index, ahead):
        out = lax.dynamic_update_slice_in_dim(
            jnp.zeros((4,) + block.shape, block.dtype), block[None], index, 0
        )
        for k in range(1, 4):
            got = lax.ppermute(block, ALL, ahead(k))
            out = lax.dynamic_update_slice_in_dim(out, got[None], lax.rem(index - k + 4, 4), 0)
        return out.reshape(-1, LEAD)

    def along_far(k):
        return [
            (place(v, c, n, f), place(v, c, n, (f + k) % 4)) for v in four for c in cores for n in four for f in four
        ]

    def along_near(k):
        return [
            (place(v, c, n, f), place(v, c, (n + k) % 4, f)) for v in four for c in cores for n in four for f in four
        ]

    own = exchange(own, far, along_far)
    own, panel = lax.optimization_barrier((own, panel))
    return exchange(own, near, along_near), panel


def on_device(covariance, weights, dual_slacks, returns, targets, sector_duals, lengths):
    tile_rows, tile_cols = covariance.shape
    rows_n, cols_n = 8, 16
    order = tile_rows * rows_n
    row_id, col_id = lax.axis_index(ROW), lax.axis_index(COL)
    row_start, col_start = row_id * tile_rows, col_id * tile_cols
    sectors_here = targets.shape[0]
    global_rows = row_start + jnp.arange(tile_rows, dtype=jnp.int32)
    global_cols = col_start + jnp.arange(tile_cols, dtype=jnp.int32)

    panel, small = lax.optimization_barrier(
        (jnp.where(col_id == 0, covariance, 0.0), jnp.stack([weights, dual_slacks, returns]))
    )
    own = lax.psum_scatter(panel, COL, scatter_dimension=0, tiled=True)
    small = lax.all_gather(small, COL, axis=0, tiled=True)
    lower_mask = global_rows[:, None] >= global_cols[None, :]
    strict_mask = global_rows[:, None] > global_cols[None, :]

    half = LEAD // 2
    second = lax.ppermute(covariance[half:LEAD], ALL, [(flat(0, 0, 0, 0), flat(0, 1, 0, 0))])
    mine = jnp.where(lax.axis_index("core") == 0, covariance[:half], second)
    mine, small = lax.optimization_barrier((mine, small))
    mine, own = spread_lead(mine, own)

    small = lax.all_gather(small, ROW, axis=0, tiled=True)
    small = small.reshape(rows_n * cols_n, 3, -1)
    full_weights, full_slacks, full_returns = (small[:, k].reshape(order) for k in range(3))
    weight_rows = lax.dynamic_slice_in_dim(full_weights, row_start, tile_rows)
    weight_cols = lax.dynamic_slice_in_dim(full_weights, col_start, tile_cols)
    row_part = jnp.sum(jnp.where(lower_mask, covariance, 0.0) * weight_cols[None, :], axis=1)
    col_part = jnp.sum(jnp.where(strict_mask, covariance, 0.0) * weight_rows[:, None], axis=0)
    lines = jnp.concatenate([col_part, row_part[:LEAD]]).reshape(1, -1)
    lines = lax.all_gather(lines, ROW, axis=0, tiled=True)
    col_sum, head_part = jnp.sum(lines[:, :tile_cols], axis=0), lines[0, tile_cols:]
    left = row_part[:tile_cols] + jnp.where(col_id == 2 * row_id, col_sum, 0.0)
    right = row_part[tile_cols:] + jnp.where(col_id == 2 * row_id + 1, col_sum, 0.0)
    head_part = head_part + jnp.where(col_id == 0, col_sum, 0.0)
    lines = jnp.concatenate([left, right, head_part]).reshape(1, -1)
    lines = lax.all_gather(lines, COL, axis=0, tiled=True)
    product = jnp.sum(lines, axis=0)

    row_lines = lax.all_gather(own, COL, axis=0, tiled=True)
    moved = lax.ppermute(
        own, ALL, [(g, (g % rows_n) * cols_n + g // rows_n) for g in range(rows_n * cols_n)]
    )
    around = [moved]
    for k in range(1, 4):
        around.append(lax.ppermute(moved, "y", [(v, (v + k) % 4) for v in range(4)]))
    diag = full_slacks / full_weights
    mean_gap = jnp.sum(full_weights * full_slacks) / order

    head_index = jnp.arange(LEAD, dtype=jnp.int32)
    other = lax.ppermute(mine, "core", [(0, 1), (1, 0)])
    head_diag = diag[:LEAD].reshape(PANELS, NB)
    lower, inverse = chol_part(functools.partial(chol_start, PANELS, SPLIT_AT), mine, other, head_diag)
    lower, inverse = chol_part(functools.partial(chol_rest, PANELS, SPLIT_AT), lower, inverse, head_diag)
    around, inverse = lax.optimization_barrier((jnp.stack(around), inverse))
    across = lax.ppermute(around, "core", [(0, 1), (1, 0)])

    sector_ends = jnp.cumsum(lengths)
    offsets = sector_ends - lengths
    sector_index = col_id * sectors_here + jnp.arange(sectors_here, dtype=jnp.int32)
    my_offsets, my_ends = jnp.take(offsets, sector_index), jnp.take(sector_ends, sector_index)
    my_sizes = jnp.take(lengths, sector_index).astype(jnp.float32)
    assets = jnp.arange(order, dtype=jnp.int32)
    inside = (assets[None, :] >= my_offsets[:, None]) & (assets[None, :] < my_ends[:, None])
    sector_resid = targets - jnp.sum(jnp.where(inside, full_weights[None, :], 0.0), axis=1) / my_sizes

    def extras(index, start, count, product_here):
        member = (index[:, None] >= offsets[None, :]) & (index[:, None] < sector_ends[None, :])
        prices = jnp.sum(jnp.where(member, sector_duals[None, :], 0.0), axis=1)
        w = lax.dynamic_slice_in_dim(full_weights, start, count)
        ret = lax.dynamic_slice_in_dim(full_returns, start, count)
        rhs = ret - product_here - prices + SIGMA_GAP * mean_gap / w
        mine = (index[:, None] >= my_offsets[None, :]) & (index[:, None] < my_ends[None, :])
        sectors = jnp.where(mine, lax.rsqrt(my_sizes)[None, :], 0.0)
        return jnp.concatenate(
            [rhs[:, None], sectors, jnp.zeros((count, 47), jnp.float32)], axis=1
        )

    head = extras(head_index, 0, LEAD, product[tile_rows:])
    body = extras(global_rows, row_start, tile_rows, product[:tile_rows])
    head = jnp.concatenate([head, jnp.zeros_like(head)], axis=1)
    xh, xl, g, solved_head = weigh(inverse, around, across, head)
    diag_cols = lax.dynamic_slice_in_dim(diag, col_start, tile_cols)[None, :]
    factored, rhs, sector_cols = update(
        row_lines, xh, xl, g, covariance, lower, body, solved_head, diag_cols, sectors_here
    )
    return factored, rhs.reshape(tile_rows), sector_cols, sector_resid


def solution(mesh):
    finer = Mesh(mesh.devices.reshape(4, 2, 4, 4), ALL)
    in_specs = (P(ROW, COL), P(ALL), P(ALL), P(ALL), P(COL), P(), P())
    out_specs = (P(ROW, COL), P(ROW), P(ROW, COL), P(COL))
    return jax.shard_map(on_device, mesh=finer, in_specs=in_specs, out_specs=out_specs, check_vma=False)
```

```python
import functools

import jax
import jax.numpy as jnp
from jax import lax
from jax.experimental import pallas as pl
from jax.experimental.pallas import tpu as pltpu
from jax.sharding import Mesh
from jax.sharding import PartitionSpec as P

NB = 128
PANELS = 8
LEAD = NB * PANELS
ROW = ("y", "core")
COL = ("z", "x")
ALL = ROW + COL
SIGMA_GAP = 0.5

NN = (((1,), (0,)), ((), ()))
NT = (((1,), (1,)), ((), ()))


def split2(x):
    hi = x.astype(jnp.bfloat16)
    lo = (x - hi.astype(jnp.float32)).astype(jnp.bfloat16)
    return hi, lo


def dot3(a, b, dims):
    ah, al = a
    bh, bl = b
    f = functools.partial(
        lax.dot_general, dimension_numbers=dims, preferred_element_type=jnp.float32
    )
    return f(ah, bh) + (f(ah, bl) + f(al, bh))


def factor_block(d_ref, r_ref):
    lane = lax.broadcasted_iota(jnp.int32, (8, NB), 1)
    sub = lax.broadcasted_iota(jnp.int32, (8, NB), 0)
    wide = lambda x: jnp.broadcast_to(x, (8, NB))
    for g in range(NB // 8):
        base = 8 * g
        head = d_ref[base : base + 8, :]
        cols = [
            jnp.where(lane == base + k, head, wide(head[:, base + k : base + k + 1])) for k in range(8)
        ]
        out = jnp.zeros((8, NB), jnp.float32)
        scale = jnp.zeros((8, NB), jnp.float32)
        for k in range(8):
            r = lax.rsqrt(wide(cols[k][k : k + 1, :]))
            rp = r * r
            m = jnp.where(sub == k, 0.0, cols[k] * rp)
            here = lane == base + k
            row = jnp.where(here, 1.0, wide(head[k : k + 1, :]))
            out = jnp.where(sub == k, row * r, out)
            scale = jnp.where(sub == k, rp, scale)
            head = jnp.where(here, jnp.where(sub == k, 1.0, 0.0), head) - m * row
            for k2 in range(k + 1, 8):
                cols[k2] = cols[k2] - m * wide(cols[k2][k : k + 1, :])
        r_ref[base : base + 8, :] = out
        head = head * scale
        rows = [wide(head[k : k + 1, :]) for k in range(8)]
        block = (lane >= base) & (lane < base + 8)
        for i in range(g + 1, NB // 8):
            cur = d_ref[8 * i : 8 * i + 8, :]
            t = [wide(cur[:, base + k : base + k + 1]) * rows[k] for k in range(8)]
            t = ((t[0] + t[1]) + (t[2] + t[3])) + ((t[4] + t[5]) + (t[6] + t[7]))
            d_ref[8 * i : 8 * i + 8, :] = jnp.where(block, 0.0, cur) - t


def stacked(pair, axis):
    return jnp.concatenate(pair, axis=axis)


def panel_steps(first, last, panels, diag_ref, l_ref, w_ref, d_ref, r_ref):
    n = panels * NB
    ri = lax.broadcasted_iota(jnp.int32, (NB, NB), 0)
    ci = lax.broadcasted_iota(jnp.int32, (NB, NB), 1)
    f = lambda a, b, dims: lax.dot_general(a, b, dims, preferred_element_type=jnp.float32)

    def step(kb, _):
        at = pl.multiple_of(kb * NB, NB)
        d = w_ref[pl.ds(at, NB), pl.ds(at, NB)]
        added = jnp.where(ri == ci, jnp.broadcast_to(diag_ref[pl.ds(kb, 1), :], (NB, NB)), 0.0)
        d_ref[...] = jnp.where(ri >= ci, d, d.T) + added
        factor_block(d_ref, r_ref)
        both = r_ref[...]
        inv = jnp.where(ri >= ci, both, 0.0)
        up = jnp.where(ri < ci, both, jnp.where(ri == ci, 1.0 / both, 0.0))
        l_ref[pl.ds(at, NB), pl.ds(at, NB)] = up.T
        invs = split2(inv)
        for k in range(first, last):

            @pl.when(kb == k)
            def _():
                lo, hi = k * NB, (k + 1) * NB
                if k:
                    w_ref[lo:hi, :lo] = dot3(invs, split2(w_ref[lo:hi, :lo]), NN)
                w_ref[lo:hi, lo:hi] = inv
                if k < panels - 1:
                    low = dot3(split2(w_ref[hi:, lo:hi]), invs, NT)
                    l_ref[hi:, lo:hi] = low
                    l_ref[lo:hi, hi:] = jnp.zeros((NB, n - hi), jnp.float32)
                    w_ref[lo:hi, hi:] = jnp.zeros((NB, n - hi), jnp.float32)
                    lh, ll = split2(low)
                    both_l, twice_l = stacked((lh, ll), 1), stacked((lh, lh), 1)
                    wh, wl = split2(w_ref[lo:hi, :hi])
                    t = f(both_l, stacked((wh, wh), 0), NN) + f(lh, wl, NN)
                    if k:
                        w_ref[hi:, :lo] -= t[:, :lo]
                    w_ref[hi:, lo:hi] = -t[:, lo:]
                    for c in range(hi, n, 2 * NB):
                        a0, a1 = c - hi, min(c + 2 * NB, n) - hi
                        t = f(both_l[a0:], twice_l[a0:a1], NT) + f(lh[a0:], ll[a0:a1], NT)
                        w_ref[c:, c : hi + a1] -= t

        return 0

    lax.fori_loop(first, last, step, 0)


def chol_start(panels, last, mine_ref, other_ref, diag_ref, l_ref, w_ref, d_ref, r_ref):
    core = lax.axis_index("core")
    span = mine_ref.shape[0]

    @pl.when(core == 0)
    def _():
        w_ref[:span] = mine_ref[...]
        w_ref[span:] = other_ref[...]

    @pl.when(core == 1)
    def _():
        w_ref[:span] = other_ref[...]
        w_ref[span:] = mine_ref[...]

    panel_steps(0, last, panels, diag_ref, l_ref, w_ref, d_ref, r_ref)


def chol_part(kernel, *args):
    n = args[0].shape[1]
    return pl.pallas_call(
        kernel,
        out_shape=[jax.ShapeDtypeStruct((n, n), jnp.float32)] * 2,
        in_specs=[pl.BlockSpec(memory_space=pltpu.VMEM)] * 3,
        out_specs=[pl.BlockSpec(memory_space=pltpu.VMEM)] * 2,
        scratch_shapes=[pltpu.VMEM((NB, NB), jnp.float32)] * 2,
        compiler_params=pltpu.CompilerParams(vmem_limit_bytes=50 * 2**20),
    )(*args)


def flat(y, core, z, x):
    return ((y * 2 + core) * 4 + z) * 4 + x


def factor_kernel(w_ref, own_ref, other_ref, e_ref, xh_ref, xl_ref, g_ref, head_ref, ah, al, mh, ml, acc):
    n, wide = LEAD, 256
    core, y, col = lax.axis_index("core"), lax.axis_index("y"), lax.axis_index(COL)
    piece = own_ref.shape[1]
    for k in range(4):
        group = 2 * lax.rem(y - k + 4, 4)
        for source, q in ((own_ref, core), (other_ref, 1 - core)):
            hi, lo = split2(source[k])
            at = pl.multiple_of((group + q) * piece, piece)
            ah[pl.ds(at, piece), :] = hi
            al[pl.ds(at, piece), :] = lo
    ri = lax.broadcasted_iota(jnp.int32, (wide, n), 0)
    ci = lax.broadcasted_iota(jnp.int32, (wide, n), 1)
    part = lambda i: pl.ds(pl.multiple_of(i * wide, wide), wide)

    def first(i, _):
        acc[...] = jnp.zeros_like(acc)

        def add(k, _):
            w = split2(w_ref[part(i), part(k)])
            acc[:, :n] += dot3(w, (ah[:, part(k)], al[:, part(k)]), NT)
            acc[:, n:] += dot3(w, split2(e_ref[part(k), :]), NN)
            return 0

        lax.fori_loop(0, i + 1, add, 0)
        m = acc[:, :n]
        m = jnp.where(col == 0, jnp.where(ri + i * wide == ci, -1.0, 0.0), m)
        mh[part(i), :n], ml[part(i), :n] = split2(m)
        m = acc[:, n:]
        head_ref[part(i), :] = m
        mh[part(i), n:], ml[part(i), n:] = split2(m)
        return 0

    def second(i, _):
        acc[...] = jnp.zeros_like(acc)

        def add(k, _):
            w = split2(w_ref[part(k), part(i)].T)
            acc[...] += dot3(w, (mh[part(k), :], ml[part(k), :]), NN)
            return 0

        lax.fori_loop(i, n // wide, add, 0)
        xh_ref[part(i), :], xl_ref[part(i), :] = split2(acc[:, :n])
        gh, gl = split2(acc[:, n:])
        g_ref[part(i), :64], g_ref[part(i), 64:] = gh[:, :64], gl[:, :64]
        return 0

    lax.fori_loop(0, n // wide, first, 0)
    lax.fori_loop(0, n // wide, second, 0)


def weigh(inverse, own, other, extra):
    n = inverse.shape[0]
    vmem = pl.BlockSpec(memory_space=pltpu.VMEM)
    return pl.pallas_call(
        factor_kernel,
        out_shape=[
            jax.ShapeDtypeStruct((n, n), jnp.bfloat16),
            jax.ShapeDtypeStruct((n, n), jnp.bfloat16),
            jax.ShapeDtypeStruct((n, NB), jnp.bfloat16),
            jax.ShapeDtypeStruct((n, NB), jnp.float32),
        ],
        in_specs=[vmem] * 4,
        out_specs=[vmem] * 4,
        scratch_shapes=[pltpu.VMEM((n, n), jnp.bfloat16)] * 2
        + [pltpu.VMEM((n, n + NB), jnp.bfloat16)] * 2
        + [pltpu.VMEM((256, n + NB), jnp.float32)],
        compiler_params=pltpu.CompilerParams(vmem_limit_bytes=56 * 2**20),
        name="weigh",
    )(inverse, own, other, extra)


def update_kernel(rows_ref, xh_ref, xl_ref, g_ref, cov_ref, low_ref, e_ref, head_ref, d_ref, out_ref, rhs_ref, sec_ref):
    block, n = rows_ref.shape
    step = pl.program_id(0)
    rows_total = pl.num_programs(0) * block
    row, col = lax.axis_index(ROW), lax.axis_index(COL)
    ah, al = split2(rows_ref[...])
    x = (xh_ref[...], xl_ref[...])
    t = dot3((ah, al), x, NN)
    f = functools.partial(
        lax.dot_general, dimension_numbers=NN, preferred_element_type=jnp.float32
    )
    g = g_ref[...]
    p, q = f(ah, g), f(al, g)
    extra = e_ref[...] - (p[:, :64] + (p[:, 64:] + q[:, :64]))
    top = (row == 0) & (step * block < LEAD)
    extra = jnp.where(top, head_ref[:, :64], extra)
    sec_ref[...] = extra[:, 1 : 1 + sec_ref.shape[1]]
    rhs_ref[...] = jnp.concatenate([extra, jnp.zeros_like(extra)], axis=1).T[0:1, :]
    ri = lax.broadcasted_iota(jnp.int32, (block, n), 0) + (row * rows_total + step * block)
    ci = lax.broadcasted_iota(jnp.int32, (block, n), 1) + col * n
    base = jnp.where(ri == ci, cov_ref[...] + d_ref[...], cov_ref[...])
    base = jnp.where(col == 0, 0.0, base)
    tile = jnp.where(ri >= ci, base - t, 0.0)
    out_ref[...] = jnp.where(top & (col == 0), low_ref[...], tile)


def update(rows, xh, xl, g, covariance, lower, extra, head, diag, sectors):
    m, n = covariance.shape
    block = 512
    last = LEAD // block - 1
    whole = lambda a: pl.BlockSpec(a.shape, lambda i: (0, 0))
    lines = lambda w: pl.BlockSpec((block, w), lambda i: (i, 0))
    ahead = lambda w: pl.BlockSpec((block, w), lambda i: (jnp.minimum(i, last), 0))
    return pl.pallas_call(
        update_kernel,
        grid=(m // block,),
        out_shape=[
            jax.ShapeDtypeStruct((m, n), jnp.float32),
            jax.ShapeDtypeStruct((1, m), jnp.float32),
            jax.ShapeDtypeStruct((m, sectors), jnp.float32),
        ],
        in_specs=[lines(n), whole(xh), whole(xl), whole(g), lines(n), ahead(n), lines(64), ahead(NB), whole(diag)],
        out_specs=[lines(n), pl.BlockSpec((1, block), lambda i: (0, i)), lines(sectors)],
        compiler_params=pltpu.CompilerParams(
            vmem_limit_bytes=56 * 2**20, dimension_semantics=("arbitrary",)
        ),
        name="update",
    )(rows, xh, xl, g, covariance, lower, extra, head, diag)


def place(y, core, near, far):
    return flat(y, core, far, near) if core == 0 else flat(y, core, near, far)


def spread_lead(half, panel):
    first = lax.axis_index("core") == 0
    z, x, y = lax.axis_index("z"), lax.axis_index("x"), lax.axis_index("y")
    near, far = jnp.where(first, x, z), jnp.where(first, z, x)
    four = range(4)
    cores = range(2)
    loads = half.reshape(4, -1, LEAD)
    bundle = loads[0]
    for k in range(1, 4):
        got = lax.ppermute(loads[k], ALL, [(place(0, c, 0, 0), place(0, c, k, 0)) for c in cores])
        bundle = jnp.where(near == k, got, bundle)
    loads = bundle.reshape(4, -1, LEAD)
    part = loads[0]
    for k in range(1, 4):
        pairs = [(place(0, c, n, 0), place(0, c, n, k)) for c in cores for n in four]
        part = jnp.where(far == k, lax.ppermute(loads[k], ALL, pairs), part)
    own = part
    for k in range(1, 4):
        pairs = [(place(0, c, n, f), place(k, c, n, f)) for c in cores for n in four for f in four]
        own = jnp.where(y == k, lax.ppermute(part, ALL, pairs), own)

    def exchange(block, index, ahead):
        out = lax.dynamic_update_slice_in_dim(
            jnp.zeros((4,) + block.shape, block.dtype), block[None], index, 0
        )
        for k in range(1, 4):
            got = lax.ppermute(block, ALL, ahead(k))
            out = lax.dynamic_update_slice_in_dim(out, got[None], lax.rem(index - k + 4, 4), 0)
        return out.reshape(-1, LEAD)

    def along_far(k):
        return [
            (place(v, c, n, f), place(v, c, n, (f + k) % 4)) for v in four for c in cores for n in four for f in four
        ]

    def along_near(k):
        return [
            (place(v, c, n, f), place(v, c, (n + k) % 4, f)) for v in four for c in cores for n in four for f in four
        ]

    own = exchange(own, far, along_far)
    own, panel = lax.optimization_barrier((own, panel))
    return exchange(own, near, along_near), panel


def on_device(covariance, weights, dual_slacks, returns, targets, sector_duals, lengths):
    tile_rows, tile_cols = covariance.shape
    rows_n, cols_n = 8, 16
    order = tile_rows * rows_n
    row_id, col_id = lax.axis_index(ROW), lax.axis_index(COL)
    row_start, col_start = row_id * tile_rows, col_id * tile_cols
    sectors_here = targets.shape[0]
    global_rows = row_start + jnp.arange(tile_rows, dtype=jnp.int32)
    global_cols = col_start + jnp.arange(tile_cols, dtype=jnp.int32)

    panel, small = lax.optimization_barrier(
        (jnp.where(col_id == 0, covariance, 0.0), jnp.stack([weights, dual_slacks, returns]))
    )
    own = lax.psum_scatter(panel, COL, scatter_dimension=0, tiled=True)
    small = lax.all_gather(small, COL, axis=0, tiled=True)
    lower_mask = global_rows[:, None] >= global_cols[None, :]
    strict_mask = global_rows[:, None] > global_cols[None, :]

    half = LEAD // 2
    second = lax.ppermute(covariance[half:LEAD], ALL, [(flat(0, 0, 0, 0), flat(0, 1, 0, 0))])
    mine = jnp.where(lax.axis_index("core") == 0, covariance[:half], second)
    mine, small = lax.optimization_barrier((mine, small))
    mine, own = spread_lead(mine, own)

    small = lax.all_gather(small, ROW, axis=0, tiled=True)
    small = small.reshape(rows_n * cols_n, 3, -1)
    full_weights, full_slacks, full_returns = (small[:, k].reshape(order) for k in range(3))
    weight_rows = lax.dynamic_slice_in_dim(full_weights, row_start, tile_rows)
    weight_cols = lax.dynamic_slice_in_dim(full_weights, col_start, tile_cols)
    row_part = jnp.sum(jnp.where(lower_mask, covariance, 0.0) * weight_cols[None, :], axis=1)
    col_part = jnp.sum(jnp.where(strict_mask, covariance, 0.0) * weight_rows[:, None], axis=0)
    lines = jnp.concatenate([col_part, row_part[:LEAD]]).reshape(1, -1)
    lines = lax.all_gather(lines, ROW, axis=0, tiled=True)
    col_sum, head_part = jnp.sum(lines[:, :tile_cols], axis=0), lines[0, tile_cols:]
    left = row_part[:tile_cols] + jnp.where(col_id == 2 * row_id, col_sum, 0.0)
    right = row_part[tile_cols:] + jnp.where(col_id == 2 * row_id + 1, col_sum, 0.0)
    head_part = head_part + jnp.where(col_id == 0, col_sum, 0.0)
    lines = jnp.concatenate([left, right, head_part]).reshape(1, -1)
    lines = lax.all_gather(lines, COL, axis=0, tiled=True)
    product = jnp.sum(lines, axis=0)

    row_lines = lax.all_gather(own, COL, axis=0, tiled=True)
    moved = lax.ppermute(
        own, ALL, [(g, (g % rows_n) * cols_n + g // rows_n) for g in range(rows_n * cols_n)]
    )
    around = [moved]
    for k in range(1, 4):
        around.append(lax.ppermute(moved, "y", [(v, (v + k) % 4) for v in range(4)]))
    diag = full_slacks / full_weights
    mean_gap = jnp.sum(full_weights * full_slacks) / order

    head_index = jnp.arange(LEAD, dtype=jnp.int32)
    other = lax.ppermute(mine, "core", [(0, 1), (1, 0)])
    head_diag = diag[:LEAD].reshape(PANELS, NB)
    lower, inverse = chol_part(functools.partial(chol_start, PANELS, PANELS), mine, other, head_diag)
    around, inverse = lax.optimization_barrier((jnp.stack(around), inverse))
    across = lax.ppermute(around, "core", [(0, 1), (1, 0)])

    sector_ends = jnp.cumsum(lengths)
    offsets = sector_ends - lengths
    sector_index = col_id * sectors_here + jnp.arange(sectors_here, dtype=jnp.int32)
    my_offsets, my_ends = jnp.take(offsets, sector_index), jnp.take(sector_ends, sector_index)
    my_sizes = jnp.take(lengths, sector_index).astype(jnp.float32)
    assets = jnp.arange(order, dtype=jnp.int32)
    inside = (assets[None, :] >= my_offsets[:, None]) & (assets[None, :] < my_ends[:, None])
    sector_resid = targets - jnp.sum(jnp.where(inside, full_weights[None, :], 0.0), axis=1) / my_sizes

    def extras(index, start, count, product_here):
        member = (index[:, None] >= offsets[None, :]) & (index[:, None] < sector_ends[None, :])
        prices = jnp.sum(jnp.where(member, sector_duals[None, :], 0.0), axis=1)
        w = lax.dynamic_slice_in_dim(full_weights, start, count)
        ret = lax.dynamic_slice_in_dim(full_returns, start, count)
        rhs = ret - product_here - prices + SIGMA_GAP * mean_gap / w
        mine = (index[:, None] >= my_offsets[None, :]) & (index[:, None] < my_ends[None, :])
        sectors = jnp.where(mine, lax.rsqrt(my_sizes)[None, :], 0.0)
        return jnp.concatenate(
            [rhs[:, None], sectors, jnp.zeros((count, 47), jnp.float32)], axis=1
        )

    head = extras(head_index, 0, LEAD, product[tile_rows:])
    body = extras(global_rows, row_start, tile_rows, product[:tile_rows])
    head = jnp.concatenate([head, jnp.zeros_like(head)], axis=1)
    xh, xl, g, solved_head = weigh(inverse, around, across, head)
    diag_cols = lax.dynamic_slice_in_dim(diag, col_start, tile_cols)[None, :]
    factored, rhs, sector_cols = update(
        row_lines, xh, xl, g, covariance, lower, body, solved_head, diag_cols, sectors_here
    )
    return factored, rhs.reshape(tile_rows), sector_cols, sector_resid


def solution(mesh):
    finer = Mesh(mesh.devices.reshape(4, 2, 4, 4), ALL)
    in_specs = (P(ROW, COL), P(ALL), P(ALL), P(ALL), P(COL), P(), P())
    out_specs = (P(ROW, COL), P(ROW), P(ROW, COL), P(COL))
    return jax.shard_map(on_device, mesh=finer, in_specs=in_specs, out_specs=out_specs, check_vma=False)
```

```python
import functools

import jax
import jax.numpy as jnp
from jax import lax
from jax.experimental import pallas as pl
from jax.experimental.pallas import tpu as pltpu
from jax.sharding import Mesh
from jax.sharding import PartitionSpec as P

NB = 128
PANELS = 8
LEAD = NB * PANELS
ROW = ("y", "core")
COL = ("z", "x")
ALL = ROW + COL
SIGMA_GAP = 0.5

NN = (((1,), (0,)), ((), ()))
NT = (((1,), (1,)), ((), ()))


def split2(x):
    hi = x.astype(jnp.bfloat16)
    lo = (x - hi.astype(jnp.float32)).astype(jnp.bfloat16)
    return hi, lo


def dot3(a, b, dims):
    ah, al = a
    bh, bl = b
    f = functools.partial(
        lax.dot_general, dimension_numbers=dims, preferred_element_type=jnp.float32
    )
    return f(ah, bh) + (f(ah, bl) + f(al, bh))


def factor_block(d_ref, r_ref):
    lane = lax.broadcasted_iota(jnp.int32, (8, NB), 1)
    sub = lax.broadcasted_iota(jnp.int32, (8, NB), 0)
    wide = lambda x: jnp.broadcast_to(x, (8, NB))
    for g in range(NB // 8):
        base = 8 * g
        head = d_ref[base : base + 8, :]
        cols = [
            jnp.where(lane == base + k, head, wide(head[:, base + k : base + k + 1])) for k in range(8)
        ]
        out = jnp.zeros((8, NB), jnp.float32)
        scale = jnp.zeros((8, NB), jnp.float32)
        for k in range(8):
            r = lax.rsqrt(wide(cols[k][k : k + 1, :]))
            rp = r * r
            m = jnp.where(sub == k, 0.0, cols[k] * rp)
            here = lane == base + k
            row = jnp.where(here, 1.0, wide(head[k : k + 1, :]))
            out = jnp.where(sub == k, row * r, out)
            scale = jnp.where(sub == k, rp, scale)
            head = jnp.where(here, jnp.where(sub == k, 1.0, 0.0), head) - m * row
            for k2 in range(k + 1, 8):
                cols[k2] = cols[k2] - m * wide(cols[k2][k : k + 1, :])
        r_ref[base : base + 8, :] = out
        head = head * scale
        rows = [wide(head[k : k + 1, :]) for k in range(8)]
        block = (lane >= base) & (lane < base + 8)
        for i in range(g + 1, NB // 8):
            cur = d_ref[8 * i : 8 * i + 8, :]
            t = [wide(cur[:, base + k : base + k + 1]) * rows[k] for k in range(8)]
            t = ((t[0] + t[1]) + (t[2] + t[3])) + ((t[4] + t[5]) + (t[6] + t[7]))
            d_ref[8 * i : 8 * i + 8, :] = jnp.where(block, 0.0, cur) - t


def stacked(pair, axis):
    return jnp.concatenate(pair, axis=axis)


def panel_steps(first, last, panels, diag_ref, l_ref, w_ref, d_ref, r_ref):
    n = panels * NB
    ri = lax.broadcasted_iota(jnp.int32, (NB, NB), 0)
    ci = lax.broadcasted_iota(jnp.int32, (NB, NB), 1)
    f = lambda a, b, dims: lax.dot_general(a, b, dims, preferred_element_type=jnp.float32)

    def step(kb, _):
        at = pl.multiple_of(kb * NB, NB)
        d = w_ref[pl.ds(at, NB), pl.ds(at, NB)]
        added = jnp.where(ri == ci, jnp.broadcast_to(diag_ref[pl.ds(kb, 1), :], (NB, NB)), 0.0)
        d_ref[...] = jnp.where(ri >= ci, d, d.T) + added
        factor_block(d_ref, r_ref)
        both = r_ref[...]
        inv = jnp.where(ri >= ci, both, 0.0)
        up = jnp.where(ri < ci, both, jnp.where(ri == ci, 1.0 / both, 0.0))
        l_ref[pl.ds(at, NB), pl.ds(at, NB)] = up.T
        invs = split2(inv)
        for k in range(first, last):

            @pl.when(kb == k)
            def _():
                lo, hi = k * NB, (k + 1) * NB
                if k:
                    w_ref[lo:hi, :lo] = dot3(invs, split2(w_ref[lo:hi, :lo]), NN)
                w_ref[lo:hi, lo:hi] = inv
                if k < panels - 1:
                    low = dot3(split2(w_ref[hi:, lo:hi]), invs, NT)
                    l_ref[hi:, lo:hi] = low
                    l_ref[lo:hi, hi:] = jnp.zeros((NB, n - hi), jnp.float32)
                    w_ref[lo:hi, hi:] = jnp.zeros((NB, n - hi), jnp.float32)
                    lh, ll = split2(low)
                    both_l, twice_l = stacked((lh, ll), 1), stacked((lh, lh), 1)
                    wh, wl = split2(w_ref[lo:hi, :hi])
                    t = f(both_l, stacked((wh, wh), 0), NN) + f(lh, wl, NN)
                    if k:
                        w_ref[hi:, :lo] -= t[:, :lo]
                    w_ref[hi:, lo:hi] = -t[:, lo:]
                    for c in range(hi, n, 2 * NB):
                        a0, a1 = c - hi, min(c + 2 * NB, n) - hi
                        t = f(both_l[a0:], twice_l[a0:a1], NT) + f(lh[a0:], ll[a0:a1], NT)
                        w_ref[c:, c : hi + a1] -= t

        return 0

    lax.fori_loop(first, last, step, 0)


def chol_start(panels, last, mine_ref, other_ref, diag_ref, l_ref, w_ref, d_ref, r_ref):
    core = lax.axis_index("core")
    span = mine_ref.shape[0]

    @pl.when(core == 0)
    def _():
        w_ref[:span] = mine_ref[...]
        w_ref[span:] = other_ref[...]

    @pl.when(core == 1)
    def _():
        w_ref[:span] = other_ref[...]
        w_ref[span:] = mine_ref[...]

    panel_steps(0, last, panels, diag_ref, l_ref, w_ref, d_ref, r_ref)


def chol_part(kernel, *args):
    n = args[0].shape[1]
    return pl.pallas_call(
        kernel,
        out_shape=[jax.ShapeDtypeStruct((n, n), jnp.float32)] * 2,
        in_specs=[pl.BlockSpec(memory_space=pltpu.VMEM)] * 3,
        out_specs=[pl.BlockSpec(memory_space=pltpu.VMEM)] * 2,
        scratch_shapes=[pltpu.VMEM((NB, NB), jnp.float32)] * 2,
        compiler_params=pltpu.CompilerParams(vmem_limit_bytes=50 * 2**20),
    )(*args)


def flat(y, core, z, x):
    return ((y * 2 + core) * 4 + z) * 4 + x


def factor_kernel(w_ref, own_ref, other_ref, e_ref, xh_ref, xl_ref, g_ref, head_ref, ah, al, mh, ml, acc):
    n, wide = LEAD, 256
    core, y, col = lax.axis_index("core"), lax.axis_index("y"), lax.axis_index(COL)
    piece = own_ref.shape[1]
    for k in range(4):
        group = 2 * lax.rem(y - k + 4, 4)
        for source, q in ((own_ref, core), (other_ref, 1 - core)):
            hi, lo = split2(source[k])
            at = pl.multiple_of((group + q) * piece, piece)
            ah[pl.ds(at, piece), :] = hi
            al[pl.ds(at, piece), :] = lo
    ri = lax.broadcasted_iota(jnp.int32, (wide, n), 0)
    ci = lax.broadcasted_iota(jnp.int32, (wide, n), 1)
    part = lambda i: pl.ds(pl.multiple_of(i * wide, wide), wide)
    deep = lambda i: pl.ds(pl.multiple_of(i * 2 * wide, 2 * wide), 2 * wide)

    def first(i, _):
        acc[...] = jnp.zeros_like(acc)

        def add(k, _):
            w = split2(w_ref[part(i), deep(k)])
            acc[:, :n] += dot3(w, (ah[:, deep(k)], al[:, deep(k)]), NT)
            acc[:, n:] += dot3(w, split2(e_ref[deep(k), :]), NN)
            return 0

        lax.fori_loop(0, i // 2 + 1, add, 0)
        m = acc[:, :n]
        m = jnp.where(col == 0, jnp.where(ri + i * wide == ci, -1.0, 0.0), m)
        mh[part(i), :n], ml[part(i), :n] = split2(m)
        m = acc[:, n:]
        head_ref[part(i), :] = m
        mh[part(i), n:], ml[part(i), n:] = split2(m)
        return 0

    def second(i, _):
        acc[...] = jnp.zeros_like(acc)

        def add(k, _):
            w = split2(w_ref[deep(k), part(i)].T)
            acc[...] += dot3(w, (mh[deep(k), :], ml[deep(k), :]), NN)
            return 0

        lax.fori_loop(i // 2, n // (2 * wide), add, 0)
        xh_ref[part(i), :], xl_ref[part(i), :] = split2(acc[:, :n])
        gh, gl = split2(acc[:, n:])
        g_ref[part(i), :64], g_ref[part(i), 64:] = gh[:, :64], gl[:, :64]
        return 0

    lax.fori_loop(0, n // wide, first, 0)
    lax.fori_loop(0, n // wide, second, 0)


def weigh(inverse, own, other, extra):
    n = inverse.shape[0]
    vmem = pl.BlockSpec(memory_space=pltpu.VMEM)
    return pl.pallas_call(
        factor_kernel,
        out_shape=[
            jax.ShapeDtypeStruct((n, n), jnp.bfloat16),
            jax.ShapeDtypeStruct((n, n), jnp.bfloat16),
            jax.ShapeDtypeStruct((n, NB), jnp.bfloat16),
            jax.ShapeDtypeStruct((n, NB), jnp.float32),
        ],
        in_specs=[vmem] * 4,
        out_specs=[vmem] * 4,
        scratch_shapes=[pltpu.VMEM((n, n), jnp.bfloat16)] * 2
        + [pltpu.VMEM((n, n + NB), jnp.bfloat16)] * 2
        + [pltpu.VMEM((256, n + NB), jnp.float32)],
        compiler_params=pltpu.CompilerParams(vmem_limit_bytes=56 * 2**20),
        name="weigh",
    )(inverse, own, other, extra)


def update_kernel(rows_ref, xh_ref, xl_ref, g_ref, cov_ref, low_ref, e_ref, head_ref, d_ref, out_ref, rhs_ref, sec_ref):
    block, n = rows_ref.shape
    step = pl.program_id(0)
    rows_total = pl.num_programs(0) * block
    row, col = lax.axis_index(ROW), lax.axis_index(COL)
    ah, al = split2(rows_ref[...])
    x = (xh_ref[...], xl_ref[...])
    t = dot3((ah, al), x, NN)
    f = functools.partial(
        lax.dot_general, dimension_numbers=NN, preferred_element_type=jnp.float32
    )
    g = g_ref[...]
    p, q = f(ah, g), f(al, g)
    extra = e_ref[...] - (p[:, :64] + (p[:, 64:] + q[:, :64]))
    top = (row == 0) & (step * block < LEAD)
    extra = jnp.where(top, head_ref[:, :64], extra)
    sec_ref[...] = extra[:, 1 : 1 + sec_ref.shape[1]]
    rhs_ref[...] = jnp.concatenate([extra, jnp.zeros_like(extra)], axis=1).T[0:1, :]
    ri = lax.broadcasted_iota(jnp.int32, (block, n), 0) + (row * rows_total + step * block)
    ci = lax.broadcasted_iota(jnp.int32, (block, n), 1) + col * n
    base = jnp.where(ri == ci, cov_ref[...] + d_ref[...], cov_ref[...])
    base = jnp.where(col == 0, 0.0, base)
    tile = jnp.where(ri >= ci, base - t, 0.0)
    out_ref[...] = jnp.where(top & (col == 0), low_ref[...], tile)


def update(rows, xh, xl, g, covariance, lower, extra, head, diag, sectors):
    m, n = covariance.shape
    block = 256
    last = LEAD // block - 1
    whole = lambda a: pl.BlockSpec(a.shape, lambda i: (0, 0))
    lines = lambda w: pl.BlockSpec((block, w), lambda i: (i, 0))
    ahead = lambda w: pl.BlockSpec((block, w), lambda i: (jnp.minimum(i, last), 0))
    return pl.pallas_call(
        update_kernel,
        grid=(m // block,),
        out_shape=[
            jax.ShapeDtypeStruct((m, n), jnp.float32),
            jax.ShapeDtypeStruct((1, m), jnp.float32),
            jax.ShapeDtypeStruct((m, sectors), jnp.float32),
        ],
        in_specs=[lines(n), whole(xh), whole(xl), whole(g), lines(n), ahead(n), lines(64), ahead(NB), whole(diag)],
        out_specs=[lines(n), pl.BlockSpec((1, block), lambda i: (0, i)), lines(sectors)],
        compiler_params=pltpu.CompilerParams(
            vmem_limit_bytes=56 * 2**20, dimension_semantics=("arbitrary",)
        ),
        name="update",
    )(rows, xh, xl, g, covariance, lower, extra, head, diag)


def place(y, core, near, far):
    return flat(y, core, far, near) if core == 0 else flat(y, core, near, far)


def spread_lead(half, panel):
    first = lax.axis_index("core") == 0
    z, x, y = lax.axis_index("z"), lax.axis_index("x"), lax.axis_index("y")
    near, far = jnp.where(first, x, z), jnp.where(first, z, x)
    four = range(4)
    cores = range(2)
    loads = half.reshape(4, -1, LEAD)
    bundle = loads[0]
    for k in range(1, 4):
        got = lax.ppermute(loads[k], ALL, [(place(0, c, 0, 0), place(0, c, k, 0)) for c in cores])
        bundle = jnp.where(near == k, got, bundle)
    loads = bundle.reshape(4, -1, LEAD)
    part = loads[0]
    for k in range(1, 4):
        pairs = [(place(0, c, n, 0), place(0, c, n, k)) for c in cores for n in four]
        part = jnp.where(far == k, lax.ppermute(loads[k], ALL, pairs), part)
    own = part
    for k in range(1, 4):
        pairs = [(place(0, c, n, f), place(k, c, n, f)) for c in cores for n in four for f in four]
        own = jnp.where(y == k, lax.ppermute(part, ALL, pairs), own)

    def exchange(block, index, ahead):
        out = lax.dynamic_update_slice_in_dim(
            jnp.zeros((4,) + block.shape, block.dtype), block[None], index, 0
        )
        for k in range(1, 4):
            got = lax.ppermute(block, ALL, ahead(k))
            out = lax.dynamic_update_slice_in_dim(out, got[None], lax.rem(index - k + 4, 4), 0)
        return out.reshape(-1, LEAD)

    def along_far(k):
        return [
            (place(v, c, n, f), place(v, c, n, (f + k) % 4)) for v in four for c in cores for n in four for f in four
        ]

    def along_near(k):
        return [
            (place(v, c, n, f), place(v, c, (n + k) % 4, f)) for v in four for c in cores for n in four for f in four
        ]

    own = exchange(own, far, along_far)
    own, panel = lax.optimization_barrier((own, panel))
    return exchange(own, near, along_near), panel


def on_device(covariance, weights, dual_slacks, returns, targets, sector_duals, lengths):
    tile_rows, tile_cols = covariance.shape
    rows_n, cols_n = 8, 16
    order = tile_rows * rows_n
    row_id, col_id = lax.axis_index(ROW), lax.axis_index(COL)
    row_start, col_start = row_id * tile_rows, col_id * tile_cols
    sectors_here = targets.shape[0]
    global_rows = row_start + jnp.arange(tile_rows, dtype=jnp.int32)
    global_cols = col_start + jnp.arange(tile_cols, dtype=jnp.int32)

    panel, small = lax.optimization_barrier(
        (jnp.where(col_id == 0, covariance, 0.0), jnp.stack([weights, dual_slacks, returns]))
    )
    own = lax.psum_scatter(panel, COL, scatter_dimension=0, tiled=True)
    small = lax.all_gather(small, COL, axis=0, tiled=True)
    lower_mask = global_rows[:, None] >= global_cols[None, :]
    strict_mask = global_rows[:, None] > global_cols[None, :]

    half = LEAD // 2
    second = lax.ppermute(covariance[half:LEAD], ALL, [(flat(0, 0, 0, 0), flat(0, 1, 0, 0))])
    mine = jnp.where(lax.axis_index("core") == 0, covariance[:half], second)
    mine, small = lax.optimization_barrier((mine, small))
    mine, own = spread_lead(mine, own)

    small = lax.all_gather(small, ROW, axis=0, tiled=True)
    small = small.reshape(rows_n * cols_n, 3, -1)
    full_weights, full_slacks, full_returns = (small[:, k].reshape(order) for k in range(3))
    weight_rows = lax.dynamic_slice_in_dim(full_weights, row_start, tile_rows)
    weight_cols = lax.dynamic_slice_in_dim(full_weights, col_start, tile_cols)
    row_part = jnp.sum(jnp.where(lower_mask, covariance, 0.0) * weight_cols[None, :], axis=1)
    col_part = jnp.sum(jnp.where(strict_mask, covariance, 0.0) * weight_rows[:, None], axis=0)
    lines = jnp.concatenate([col_part, row_part[:LEAD]]).reshape(1, -1)
    lines = lax.all_gather(lines, ROW, axis=0, tiled=True)
    col_sum, head_part = jnp.sum(lines[:, :tile_cols], axis=0), lines[0, tile_cols:]
    left = row_part[:tile_cols] + jnp.where(col_id == 2 * row_id, col_sum, 0.0)
    right = row_part[tile_cols:] + jnp.where(col_id == 2 * row_id + 1, col_sum, 0.0)
    head_part = head_part + jnp.where(col_id == 0, col_sum, 0.0)
    lines = jnp.concatenate([left, right, head_part]).reshape(1, -1)
    lines = lax.all_gather(lines, COL, axis=0, tiled=True)
    product = jnp.sum(lines, axis=0)

    row_lines = lax.all_gather(own, COL, axis=0, tiled=True)
    moved = lax.ppermute(
        own, ALL, [(g, (g % rows_n) * cols_n + g // rows_n) for g in range(rows_n * cols_n)]
    )
    around = [moved]
    for k in range(1, 4):
        around.append(lax.ppermute(moved, "y", [(v, (v + k) % 4) for v in range(4)]))
    diag = full_slacks / full_weights
    mean_gap = jnp.sum(full_weights * full_slacks) / order

    head_index = jnp.arange(LEAD, dtype=jnp.int32)
    other = lax.ppermute(mine, "core", [(0, 1), (1, 0)])
    head_diag = diag[:LEAD].reshape(PANELS, NB)
    lower, inverse = chol_part(functools.partial(chol_start, PANELS, PANELS), mine, other, head_diag)
    around, inverse = lax.optimization_barrier((jnp.stack(around), inverse))
    across = lax.ppermute(around, "core", [(0, 1), (1, 0)])

    sector_ends = jnp.cumsum(lengths)
    offsets = sector_ends - lengths
    sector_index = col_id * sectors_here + jnp.arange(sectors_here, dtype=jnp.int32)
    my_offsets, my_ends = jnp.take(offsets, sector_index), jnp.take(sector_ends, sector_index)
    my_sizes = jnp.take(lengths, sector_index).astype(jnp.float32)
    assets = jnp.arange(order, dtype=jnp.int32)
    inside = (assets[None, :] >= my_offsets[:, None]) & (assets[None, :] < my_ends[:, None])
    sector_resid = targets - jnp.sum(jnp.where(inside, full_weights[None, :], 0.0), axis=1) / my_sizes

    def extras(index, start, count, product_here):
        member = (index[:, None] >= offsets[None, :]) & (index[:, None] < sector_ends[None, :])
        prices = jnp.sum(jnp.where(member, sector_duals[None, :], 0.0), axis=1)
        w = lax.dynamic_slice_in_dim(full_weights, start, count)
        ret = lax.dynamic_slice_in_dim(full_returns, start, count)
        rhs = ret - product_here - prices + SIGMA_GAP * mean_gap / w
        mine = (index[:, None] >= my_offsets[None, :]) & (index[:, None] < my_ends[None, :])
        sectors = jnp.where(mine, lax.rsqrt(my_sizes)[None, :], 0.0)
        return jnp.concatenate(
            [rhs[:, None], sectors, jnp.zeros((count, 47), jnp.float32)], axis=1
        )

    head = extras(head_index, 0, LEAD, product[tile_rows:])
    body = extras(global_rows, row_start, tile_rows, product[:tile_rows])
    head = jnp.concatenate([head, jnp.zeros_like(head)], axis=1)
    xh, xl, g, solved_head = weigh(inverse, around, across, head)
    diag_cols = lax.dynamic_slice_in_dim(diag, col_start, tile_cols)[None, :]
    factored, rhs, sector_cols = update(
        row_lines, xh, xl, g, covariance, lower, body, solved_head, diag_cols, sectors_here
    )
    return factored, rhs.reshape(tile_rows), sector_cols, sector_resid


def solution(mesh):
    finer = Mesh(mesh.devices.reshape(4, 2, 4, 4), ALL)
    in_specs = (P(ROW, COL), P(ALL), P(ALL), P(ALL), P(COL), P(), P())
    out_specs = (P(ROW, COL), P(ROW), P(ROW, COL), P(COL))
    return jax.shard_map(on_device, mesh=finer, in_specs=in_specs, out_specs=out_specs, check_vma=False)
```
